32 devices in a mesh: gx: 4 (over y, x), gy: 4 (over z), gz: 2 (over core).
Axes of the slice: x: 2, y: 2, z: 4, core: 2. Of those that a mesh axis runs over, the one named last changes fastest.
Arguments:
- a_blocks: float32 [1664, 7, 128, 128], P(('gx', 'gy', 'gz')), as said below
- block_cols: int32 [1664, 7], P(('gx', 'gy', 'gz')), may hold values from 0 to 363, as said below
- agg_ids: int32 [1664], P(('gx', 'gy', 'gz')), may hold values from 0 to 51, as said below
- agg_counts: int32 [32], P(('gx', 'gy', 'gz')), may hold values from 1 to 52, as said below
- p0_blocks: float32 [1664, 6, 128], P(('gx', 'gy', 'gz')), may hold values from -6 to 6
- start_vec: float32 [1664, 128], P(('gx', 'gy', 'gz'))
Outputs:
- p_blocks: float32 [1664, 7, 6, 128], P(('gx', 'gy', 'gz'))
- p_cols: int32 [1664, 7], P(('gx', 'gy', 'gz'))
- power_vec: float32 [1664, 128], P(('gx', 'gy', 'gz'))
The draws below stay inside these ranges and needn't reach their ends.
Inputs may be any that keep to these rules, and one draw needn't show every extreme that they name: `block_cols`: entry 0 of each block row names the row itself; every neighbour that an entry names exists. `agg_ids`: below the count of the row's own subdomain. `agg_counts`: some subdomain has 52 aggregates. `a_blocks`: block 0 of each block row has a positive diagonal.
All inputs are finite; a program needn't handle non-finite values.
Results may differ from the reference program's by a relative error of at most 0.0003.
Values sent between devices are 32-bit elements; how exact they have to be, the bound alone decides.
A program may use at most 128 MiB of HBM per device.

```python
import jax
import jax.numpy as jnp
from jax import lax

B = 128
NS = 6
K = 7
BR = 52
ITERS = 8
BLOCKS = 1664
N_GX = 4
N_GY = 4
N_GZ = 2


def counts_helper(key):
    device_count = N_GX * N_GY * N_GZ
    per_device = jax.random.randint(jax.random.fold_in(key, 11), (device_count,), 1, BR + 1)
    chosen = jax.random.randint(jax.random.fold_in(key, 12), (), 0, device_count)
    return jnp.where(jnp.arange(device_count) == chosen, BR, per_device).astype(jnp.int32)


def draw_agg_counts(key, part):
    return counts_helper(key)


def draw_agg_ids(key, part):
    counted = jnp.repeat(counts_helper(key), BR)
    return jax.random.randint(jax.random.fold_in(key, 13), (BLOCKS,), 0, counted).astype(jnp.int32)


def draw_block_cols(key, part):
    blocks_all = jnp.arange(BLOCKS)
    device_index = blocks_all // BR
    own_row = blocks_all % BR
    coord_x = device_index // (N_GY * N_GZ)
    coord_y = device_index // N_GZ % N_GY
    coord_z = device_index % N_GZ
    exists = jnp.stack([coord_x > 0, coord_x < N_GX - 1, coord_y > 0, coord_y < N_GY - 1, coord_z > 0, coord_z < N_GZ - 1], axis=1)
    chosen = jax.random.randint(jax.random.fold_in(key, 21), (BLOCKS, 6), 0, 2)
    remote_row = jax.random.randint(jax.random.fold_in(key, 22), (BLOCKS, 6), 0, BR)
    local_row = jax.random.randint(jax.random.fold_in(key, 23), (BLOCKS, 6), 0, BR)
    direction = jnp.arange(6)[None, :]
    use_remote = (chosen == 1) & exists
    picked = jnp.where(use_remote, BR + direction * BR + remote_row, local_row)
    return jnp.concatenate([own_row[:, None], picked], axis=1).astype(jnp.int32)


def draw_a_blocks(key, part):
    device_index = (jnp.arange(BLOCKS) // BR).astype(jnp.float32)
    device_count = N_GX * N_GY * N_GZ
    strength = 0.3 + 1.2 * device_index / max(device_count - 1, 1)
    noise = jax.random.normal(jax.random.fold_in(key, 31), (BLOCKS, K, B, B), jnp.float32)
    diagonal = jax.random.uniform(jax.random.fold_in(key, 32), (BLOCKS, B), jnp.float32, 1.0, 2.0)
    identity = jnp.eye(B, dtype=jnp.float32)
    inner = noise[:, 0] * (0.4 / B ** 0.5) * (1.0 - identity) + identity * diagonal[:, :, None]
    outer = noise[:, 1:] * (strength[:, None, None, None] / (6.0 * B) ** 0.5)
    return jnp.concatenate([inner[:, None], outer], axis=1)


def draw_start_vec(key, part):
    device_index = (jnp.arange(BLOCKS) // BR).astype(jnp.float32)
    device_count = N_GX * N_GY * N_GZ
    ramp = device_index / max(device_count - 1, 1)
    values = jax.random.normal(jax.random.fold_in(key, 41), (BLOCKS, B), jnp.float32)
    return values * (1.0 + 2.0 * ramp)[:, None]


def block_levels(own_key, shape, shards, smallest, top_value):
    loudness, own = 1.0, jax.random.fold_in(own_key, 6)
    for dim, blocks in shards:
        heights = jnp.exp(jax.random.uniform(jax.random.fold_in(own, dim), (blocks,), jnp.float32, smallest / len(shards), top_value / len(shards)))
        loudness = loudness * jnp.repeat(heights, shape[dim] // blocks).reshape([-1 if axis == dim else 1 for axis in range(len(shape))])
    return loudness


def gaussian(rng, shape, deviation, bound, split=(), kind=jnp.bfloat16):
    values = jax.random.normal(rng, shape, jnp.float32) * deviation
    if len(split) > 0:
        values = block_levels(rng, shape, split, -0.22, 0.18) * values
    return jnp.clip(values, min=-bound, max=bound).astype(kind)


def setup_inputs(seed: int = 0) -> dict:
    keys = jax.random.split(jax.random.key(seed), 7)
    a_blocks = draw_a_blocks(jax.random.fold_in(keys[6], 71), 0)
    block_cols = draw_block_cols(jax.random.fold_in(keys[6], 71), 0)
    agg_ids = draw_agg_ids(jax.random.fold_in(keys[6], 71), 0)
    agg_counts = draw_agg_counts(jax.random.fold_in(keys[6], 71), 0)
    p0_blocks = gaussian(keys[4], (BLOCKS, NS, B), 1.0, 6.0, ((0, 32),), jnp.float32)
    start_vec = draw_start_vec(jax.random.fold_in(keys[6], 71), 0)
    return {"a_blocks": a_blocks, "block_cols": block_cols, "agg_ids": agg_ids, "agg_counts": agg_counts, "p0_blocks": p0_blocks, "start_vec": start_vec}


precise_mode = lax.Precision.HIGHEST

def global_rows(block_cols):
    device_count = N_GX * N_GY * N_GZ
    shaped = block_cols.reshape(device_count, BR, K)
    device_index = jnp.arange(device_count, dtype=jnp.int32)[:, None, None]
    strides = jnp.array([-N_GY * N_GZ, N_GY * N_GZ, -N_GZ, N_GZ, -1, 1], dtype=jnp.int32)
    beyond = shaped - BR
    direction = jnp.clip(beyond // BR, 0, 5)
    neighbour_row = beyond % BR
    remote = (device_index + strides[direction]) * BR + neighbour_row
    own_rows = device_index * BR + shaped
    return jnp.where(shaped < BR, own_rows, remote).reshape(device_count * BR, K).astype(jnp.int32)

def reference(a_blocks, block_cols, agg_ids, agg_counts, p0_blocks, start_vec):
    target = global_rows(block_cols)
    diag_values = jnp.diagonal(a_blocks[:, 0], axis1=1, axis2=2)

    def operate(vector):
        picked = vector[target]
        mixed = jnp.einsum('bkij,bkj->bi', a_blocks, picked, precision=precise_mode)
        return mixed / diag_values
    previous = start_vec
    current = start_vec
    for turn_index in range(ITERS):
        previous = current
        current = operate(current)
    last_norm = jnp.sqrt(jnp.sum(current * current))
    spectral = last_norm / jnp.sqrt(jnp.sum(previous * previous))
    power_vec = current * (jnp.sqrt(jnp.float32(BLOCKS * B)) / last_norm)
    damping = 4.0 / (3.0 * spectral)
    picked_p0 = p0_blocks[target]
    product = jnp.einsum('bksj,bkij->bksi', picked_p0, a_blocks, precision=precise_mode)
    smoothed = -(damping / diag_values)[:, None, None, :] * product
    p_blocks = smoothed.at[:, 0].add(p0_blocks)
    offsets = (jnp.cumsum(agg_counts) - agg_counts).astype(jnp.int32)
    p_cols = NS * (offsets[target // BR] + agg_ids[target])
    return (p_blocks, p_cols.astype(jnp.int32), power_vec)
```

```python
import functools

import jax
import jax.numpy as jnp
from jax import lax
from jax.experimental import pallas as pl
from jax.experimental.pallas import tpu as pltpu
from jax.sharding import PartitionSpec as P

ITERS = 8
AXES = ("gx", "gy", "gz")
MESH = pl.DeviceIdType.MESH
NT = (((1,), (1,)), ((), ()))


def split_bf16(x):
    hi = x.astype(jnp.bfloat16)
    lo = (x - hi.astype(jnp.float32)).astype(jnp.bfloat16)
    return jnp.concatenate([hi, lo], axis=1)


def kernel(sizes, plan, a_hbm, cols_s, cols_v, ids_v, count_s, p0_hbm, start_v,
           q_hbm, pcols_v, power_v, by_v,
           q_v, a_v, va, vb, p_t, diag, w_t, s_v, hold, meta, sums, meta_own, sums_own,
           a_sem, p0_sem, q_sem, v_send, v_recv, p_send, p_recv, m_send, m_recv, s_send, s_recv):
    nx, ny, nz = sizes
    n = nx * ny * nz
    rows, blocks, width, _ = a_v.shape
    ns = p0_hbm.shape[0]
    slot = p_t.shape[1] // 7
    ix, iy, iz = (lax.axis_index(a) for a in AXES)
    me = (ix * ny + iy) * nz + iz
    load, group, vpu = plan
    pairs = (group - vpu) // 2
    f32 = jnp.float32

    def a_copy(g):
        return pltpu.make_async_copy(
            a_hbm.at[pl.ds(g * load, load)], a_v.at[pl.ds(g * load, load)], a_sem.at[g])

    p0_copy = pltpu.make_async_copy(p0_hbm, p_t.at[:, pl.ds(0, rows)], p0_sem)
    p0_copy.start()
    for g in range(rows // load):
        a_copy(g).start()

    others = []
    for dx in range(nx):
        for dy in range(ny):
            for dz in range(nz):
                if dx or dy or dz:
                    others.append({"gx": lax.rem(ix + dx, nx), "gy": lax.rem(iy + dy, ny),
                                   "gz": lax.rem(iz + dz, nz)})

    barrier = pltpu.get_barrier_semaphore()
    for where in others:
        pl.semaphore_signal(barrier, inc=1, device_id=where, device_id_type=MESH)

    for r in range(rows):
        va[r] = start_v[r:r + 1]
    meta_own[0:1] = jnp.full((1, width), count_s[0], jnp.int32)
    meta_own[0:1, 0:rows] = ids_v[...]
    meta[pl.ds(me, 1)] = meta_own[...][None]
    pl.semaphore_wait(barrier, n - 1)

    sides = []
    for axis, (name, count, at) in enumerate(zip(AXES, sizes, (ix, iy, iz))):
        if count > 1:
            sides.append((2 * axis + 1, 2 * axis + 2, at > 0, {name: at - 1}))
            sides.append((2 * axis + 2, 2 * axis + 1, at < count - 1, {name: at + 1}))

    tables = (va, vb)

    def v_copy(turn, mine, theirs, where, at, size):
        table = tables[turn]
        return pltpu.make_async_remote_copy(
            src_ref=table.at[pl.ds(at, size)],
            dst_ref=table.at[pl.ds(theirs * rows + at, size)],
            send_sem=v_send.at[turn, mine], recv_sem=v_recv.at[turn, theirs],
            device_id=where, device_id_type=MESH)

    def v_start(turn, at, size):
        for mine, theirs, exists, where in sides:
            @pl.when(exists)
            def _():
                v_copy(turn, mine, theirs, where, at, size).start()

    def v_wait(turn):
        for mine, theirs, exists, where in sides:
            @pl.when(exists)
            def _():
                v_copy(turn, mine, theirs, where, 0, rows).wait_send()
                v_copy(turn, theirs, mine, where, 0, rows).wait_recv()

    def p_copy(mine, theirs, where, at, size):
        return pltpu.make_async_remote_copy(
            src_ref=p_t.at[pl.ds(at, size), pl.ds(0, rows)],
            dst_ref=p_t.at[pl.ds(at, size), pl.ds(theirs * slot, rows)],
            send_sem=p_send.at[mine], recv_sem=p_recv.at[theirs],
            device_id=where, device_id_type=MESH)

    def p_start(at, size):
        for mine, theirs, exists, where in sides:
            @pl.when(exists)
            def _():
                p_copy(mine, theirs, where, at, size).start()

    def p_wait():
        for mine, theirs, exists, where in sides:
            @pl.when(exists)
            def _():
                p_copy(mine, theirs, where, 0, ns).wait_send()
                p_copy(theirs, mine, where, 0, ns).wait_recv()

    def spread(own, table, send_sem, recv_sem):
        for where in others:
            pltpu.make_async_remote_copy(
                src_ref=own, dst_ref=table.at[me], send_sem=send_sem, recv_sem=recv_sem,
                device_id=where, device_id_type=MESH).start()

    def spread_wait(table, send_sem, recv_sem):
        part = table.at[pl.ds(0, n - 1)]
        pltpu.make_async_copy(part, part, send_sem).wait()
        pltpu.make_async_copy(part, part, recv_sem).wait()

    v_start(0, 0, rows)
    spread(meta_own, meta, m_send, m_recv)
    p0_copy.wait()
    early = max(1, 2 * ns // 3)
    p_start(0, early)
    v_wait(0)

    lanes = lax.broadcasted_iota(jnp.int32, (width, width), 1)
    late = hold.shape[0]

    def lane_sum(total):
        return jnp.sum(total, axis=1, keepdims=True)

    def mix(turn, b):
        src = tables[1 - turn]
        total = a_v[b, 0] * src[b]
        for k in range(1, blocks):
            total = total + a_v[b, k] * src[cols_s[k, b]]
        return total

    def pair(turn, g, p):
        src = tables[1 - turn]
        b = g * group + vpu + 2 * p
        x = jnp.concatenate(
            [jnp.concatenate([src[b + i] if k == 0 else src[cols_s[k, b + i]]
                              for k in range(blocks)], axis=1) for i in range(2)], axis=0)
        hi = x.astype(jnp.bfloat16).astype(f32)
        left = jnp.concatenate([hi, x - hi, jnp.zeros((4, x.shape[1]), f32)], axis=0).astype(jnp.bfloat16)
        left = jnp.concatenate([left, left], axis=1)
        out = jnp.dot(left, w_t[g * pairs + p], preferred_element_type=f32)
        out = out[0:2] + out[2:4]
        for i in range(2):
            r = vpu + 2 * p + i
            tables[turn][b + i] = out[i:i + 1, i * width:(i + 1) * width] / diag[b + i]

    def mix_block(turn, g, size, count, first):
        if not first:
            for p in range(pairs):
                pair(turn, g, p)
        packed = jnp.zeros((width, width), f32)
        for r in range(count):
            b = g * size + r
            total = mix(turn, b)
            if r < count - late:
                packed = jnp.where(lanes == r, lane_sum(total), packed)
            else:
                hold[r - (count - late)] = total
            if first:
                eye = lanes == lax.broadcasted_iota(jnp.int32, (width, width), 0)
                diag[b] = jnp.sum(jnp.where(eye, a_v[b, 0], 0.0), axis=0, keepdims=True)
        s_v[...] = packed

    def finish_block(turn, g, size, count):
        packed = s_v[...]
        for i in range(late):
            packed = jnp.where(lanes == count - late + i, lane_sum(hold[i]), packed)
        out = packed.T
        for r in range(count):
            b = g * size + r
            tables[turn][b] = out[r:r + 1] / diag[b]

    def operate(turn, first, send):
        size, count = (load, load) if first else (group, vpu)
        if first:
            a_copy(0).wait()
        mix_block(turn, 0, size, count, first)

        def body(g, c):
            if first:
                a_copy(g).wait()
            finish_block(turn, g - 1, size, count)
            mix_block(turn, g, size, count, first)
            if send:
                v_start(turn, (g - 1) * size, size)
            return c

        lax.fori_loop(1, rows // size, body, 0)
        finish_block(turn, rows // size - 1, size, count)
        if send:
            v_start(turn, rows - size, size)

    def turn_over(i, c):
        b = i // pairs * group + vpu + 2 * lax.rem(i, pairs)
        for k in range(blocks):
            x = jnp.concatenate([a_v[b, k].T, a_v[b + 1, k].T], axis=1)
            hi = x.astype(jnp.bfloat16)
            lo = (x - hi.astype(f32)).astype(jnp.bfloat16)
            w_t[i, k * width:(k + 1) * width] = hi
            w_t[i, (blocks + k) * width:(blocks + k + 1) * width] = lo
        return c

    def product(b, c):
        for k in range(blocks):
            at = b
            if k:
                col = cols_s[k, b]
                at = col + (slot - rows) * (col // rows)
            p = p_t[:, at, :]
            p = jnp.concatenate([p, jnp.zeros((8 - ns % 8, width), f32)], axis=0)
            hi = p.astype(jnp.bfloat16).astype(f32)
            left = jnp.concatenate([hi, p - hi], axis=0).astype(jnp.bfloat16)
            left = jnp.concatenate([left, left], axis=1)
            out = lax.dot_general(left, split_bf16(a_v[b, k]), NT, preferred_element_type=f32)
            half = out.shape[0] // 2
            q_v[k, :, b, :] = (out[:half] + out[half:])[:ns]
        return c

    def columns():
        counts = meta[...][:, :, width - 1:]
        owner = lax.broadcasted_iota(jnp.int32, counts.shape, 0)
        slots = [(jnp.bool_(True), me)]
        for (name, count, at, stride) in zip(AXES, sizes, (ix, iy, iz), (ny * nz, nz, 1)):
            slots.append((at > 0, me - stride))
            slots.append((at < count - 1, me + stride))
        entries = []
        for exists, d in slots:
            d = jnp.where(exists, d, me)
            offset = jnp.sum(jnp.where(owner < d, counts, 0).astype(f32), axis=0)
            entries.append(meta[d].astype(f32) + offset)
        entries.append(jnp.zeros((1, width), f32))
        table = jnp.concatenate(entries, axis=0).T
        row = lax.broadcasted_iota(jnp.int32, (rows, rows), 0)
        for k in range(blocks):
            cols = cols_v[k:k + 1]
            found = jnp.zeros((rows, rows), f32)
            for s in range(len(slots)):
                found = found + jnp.where(cols - s * rows == row, table[:rows, s:s + 1], 0.0)
            pcols_v[k:k + 1] = (jnp.sum(found, axis=0, keepdims=True) * ns).astype(jnp.int32)

    def squares(turn):
        own = tables[turn][0:rows]
        return jnp.sum(jnp.sum(own * own, axis=0), axis=1, keepdims=True)

    q_copy = pltpu.make_async_copy(q_v, q_hbm, q_sem)
    operate(1, True, True)
    p_start(early, ns - early)
    lax.fori_loop(0, w_t.shape[0], turn_over, 0)
    spread_wait(meta, m_send, m_recv)
    columns()
    v_wait(1)

    def step(t, turn):
        operate(turn, False, True)

        @pl.when(t == 2)
        def _():
            p_wait()

        lax.fori_loop(rows * (t - 2) // (ITERS - 2), rows * (t - 1) // (ITERS - 2), product, 0)

        @pl.when(t == ITERS - 1)
        def _():
            q_copy.start()

        v_wait(turn)

    def steps(i, c):
        for turn in range(2):
            step(2 * i + turn, turn)
        return c

    lax.fori_loop(1, ITERS // 2, steps, 0)
    before = squares((ITERS - 1) % 2)
    operate(ITERS % 2, False, False)

    lane = lax.broadcasted_iota(jnp.int32, (1, width), 1)
    sums_own[...] = jnp.where(lane == 0, before, jnp.where(lane == 1, squares(ITERS % 2), 0.0))
    sums[pl.ds(me, 1)] = sums_own[...][None]
    spread(sums_own, sums, s_send, s_recv)
    spread_wait(sums, s_send, s_recv)
    totals = jnp.sum(sums[...], axis=0)
    total_before = jnp.sum(jnp.where(lane == 0, totals, 0.0), axis=1, keepdims=True)
    total_last = jnp.sum(jnp.where(lane == 1, totals, 0.0), axis=1, keepdims=True)
    last_norm = jnp.sqrt(total_last)
    spectral = last_norm / jnp.sqrt(total_before)
    damping = 4.0 / (3.0 * spectral)
    factor = jnp.sqrt(jnp.full((1, 1), n * rows * width, f32)) / last_norm
    for r in range(rows):
        power_v[r:r + 1] = tables[ITERS % 2][r] * factor

    by_v[...] = -(damping / jnp.concatenate([diag[r] for r in range(rows)], axis=0))
    q_copy.wait()


def scale_kernel(q, p0, by, cols, power, p_out, cols_out, power_out):
    cols_out[...] = cols[...]
    power_out[...] = power[...]
    factor = by[...]
    for k in range(q.shape[0]):
        for c in range(q.shape[1]):
            scaled = factor * q[k, c]
            p_out[k, c] = scaled + p0[c] if k == 0 else scaled


def solution(mesh):
    sizes = tuple(mesh.shape[a] for a in AXES)
    n = sizes[0] * sizes[1] * sizes[2]

    def local(a_blocks, block_cols, agg_ids, agg_counts, p0_blocks, start_vec):
        rows, blocks, width, _ = a_blocks.shape
        ns = p0_blocks.shape[1]
        load = next(g for g in (13, 4, 2, 1) if rows % g == 0)
        group = 2 * load if rows % (2 * load) == 0 else load
        vpu = group - group * 4 // 13 // 2 * 2
        late = min(3, load, vpu)
        vmem = pl.BlockSpec(memory_space=pltpu.VMEM)
        smem = pl.BlockSpec(memory_space=pltpu.SMEM)
        dma = pltpu.SemaphoreType.DMA
        f32 = jnp.float32
        assert rows < width
        p0_planes = p0_blocks.transpose(1, 0, 2)
        product, cols, power, by = pl.pallas_call(
            functools.partial(kernel, sizes, (load, group, vpu)),
            out_shape=(
                jax.ShapeDtypeStruct((blocks, ns, rows, width), f32),
                jax.ShapeDtypeStruct((blocks, rows), jnp.int32),
                jax.ShapeDtypeStruct((rows, width), f32),
                jax.ShapeDtypeStruct((rows, width), f32),
            ),
            in_specs=[pl.BlockSpec(memory_space=pl.ANY), smem, vmem, vmem, smem, pl.BlockSpec(memory_space=pl.ANY), vmem],
            out_specs=(pl.BlockSpec(memory_space=pl.ANY), vmem, vmem, vmem),
            scratch_shapes=[
                pltpu.VMEM((blocks, ns, rows, width), f32),
                pltpu.VMEM((rows, blocks, width, width), f32),
                pltpu.VMEM((7 * rows, 1, width), f32),
                pltpu.VMEM((7 * rows, 1, width), f32),
                pltpu.VMEM((ns, 7 * (-(-rows // 8) * 8), width), f32),
                pltpu.VMEM((rows, 1, width), f32),
                pltpu.VMEM((rows // group * ((group - vpu) // 2), 2 * blocks * width, 2 * width), jnp.bfloat16),
                pltpu.VMEM((width, width), f32),
                pltpu.VMEM((late, width, width), f32),
                pltpu.VMEM((n, 1, width), jnp.int32),
                pltpu.VMEM((n, 1, width), f32),
                pltpu.VMEM((1, width), jnp.int32),
                pltpu.VMEM((1, width), f32),
                dma((rows // load,)), dma, dma,
                dma((2, 7)), dma((2, 7)), dma((7,)), dma((7,)),
                dma, dma, dma, dma,
            ],
            compiler_params=pltpu.CompilerParams(
                collective_id=0, has_side_effects=True, vmem_limit_bytes=56 * 1024 * 1024),
        )(a_blocks, block_cols.T, block_cols.T, agg_ids[None], agg_counts,
          p0_planes, start_vec)
        product, cols, power = pl.pallas_call(
            scale_kernel,
            out_shape=(
                jax.ShapeDtypeStruct(product.shape, f32),
                jax.ShapeDtypeStruct(cols.shape, jnp.int32),
                jax.ShapeDtypeStruct(power.shape, f32),
            ),
            in_specs=[vmem] * 5,
            out_specs=(vmem, vmem, vmem),
        )(product, p0_planes, by, cols, power)
        return product.transpose(2, 0, 1, 3), cols.T, power

    part = P(AXES)
    return jax.shard_map(
        local, mesh=mesh, in_specs=(part,) * 6, out_specs=(part,) * 3, check_vma=False)
```

```python
import functools

import jax
import jax.numpy as jnp
from jax import lax
from jax.experimental import pallas as pl
from jax.experimental.pallas import tpu as pltpu
from jax.sharding import PartitionSpec as P

ITERS = 8
SPREAD = ITERS - 3
AXES = ("gx", "gy", "gz")
MESH = pl.DeviceIdType.MESH
NT = (((1,), (1,)), ((), ()))


def split_bf16(x):
    hi = x.astype(jnp.bfloat16)
    lo = (x - hi.astype(jnp.float32)).astype(jnp.bfloat16)
    return jnp.concatenate([hi, lo], axis=1)


def kernel(sizes, plan, a_hbm, cols_hbm, ids_hbm, count_hbm, p0_hbm, start_hbm,
           q_v, own_v, pcols_v, power_v, by_v,
           cols_s, cols_v, ids_v, count_s, start_v, a_v, va, vb, p_t, diag, w_t, s_v, hold, meta, sums, meta_own, sums_own,
           a_sem, p0_sem, in_sem, v_send, v_recv, p_send, p_recv, m_send, m_recv, s_send, s_recv):
    nx, ny, nz = sizes
    n = nx * ny * nz
    rows, blocks, width, _ = a_v.shape
    ns = p0_hbm.shape[0]
    slot = p_t.shape[1] // 7
    ix, iy, iz = (lax.axis_index(a) for a in AXES)
    me = (ix * ny + iy) * nz + iz
    load, group, vpu = plan
    pairs = (group - vpu) // 2
    f32 = jnp.float32

    def a_copy(g):
        return pltpu.make_async_copy(
            a_hbm.at[pl.ds(g * load, load)], a_v.at[pl.ds(g * load, load)], a_sem.at[g])

    p0_copy = pltpu.make_async_copy(p0_hbm, p_t.at[:, pl.ds(0, rows)], p0_sem)
    inputs = [pltpu.make_async_copy(a, b, in_sem.at[i]) for i, (a, b) in enumerate((
        (start_hbm, start_v), (ids_hbm, ids_v), (count_hbm, count_s), (cols_hbm, cols_s), (cols_hbm, cols_v)))]
    for copy in inputs:
        copy.start()
    p0_copy.start()
    for g in range(rows // load):
        a_copy(g).start()

    others = []
    for dx in range(nx):
        for dy in range(ny):
            for dz in range(nz):
                if dx or dy or dz:
                    others.append(((dx > 0) + (dy > 0), {
                        "gx": lax.rem(ix + dx, nx), "gy": lax.rem(iy + dy, ny), "gz": lax.rem(iz + dz, nz)}))
    others = [where for _, where in sorted(others, key=lambda o: -o[0])]

    sides = []
    for axis, (name, count, at) in enumerate(zip(AXES, sizes, (ix, iy, iz))):
        if count > 1:
            sides.append((2 * axis + 1, 2 * axis + 2, at > 0, {name: at - 1}))
            sides.append((2 * axis + 2, 2 * axis + 1, at < count - 1, {name: at + 1}))

    near = nx + ny + nz - 3 <= SPREAD + 2
    barrier = pltpu.get_barrier_semaphore()
    if near:
        for _, _, exists, where in sides:
            @pl.when(exists)
            def _():
                pl.semaphore_signal(barrier, inc=1, device_id=where, device_id_type=MESH)
    else:
        for where in others:
            pl.semaphore_signal(barrier, inc=1, device_id=where, device_id_type=MESH)

    for copy in inputs:
        copy.wait()
    for r in range(rows):
        va[r] = start_v[r:r + 1]
    meta_own[0:1] = jnp.full((1, width), count_s[0], jnp.int32)
    meta_own[0:1, 0:rows] = ids_v[...]
    meta[pl.ds(me, 1)] = meta_own[...][None]
    if near:
        pl.semaphore_wait(barrier, sum(exists.astype(jnp.int32) for _, _, exists, _ in sides))
    else:
        pl.semaphore_wait(barrier, n - 1)

    tables = (va, vb)

    def v_copy(turn, mine, theirs, where, at, size):
        table = tables[turn]
        return pltpu.make_async_remote_copy(
            src_ref=table.at[pl.ds(at, size)],
            dst_ref=table.at[pl.ds(theirs * rows + at, size)],
            send_sem=v_send.at[turn, mine], recv_sem=v_recv.at[turn, theirs],
            device_id=where, device_id_type=MESH)

    def v_start(turn, at, size):
        for mine, theirs, exists, where in sides:
            @pl.when(exists)
            def _():
                v_copy(turn, mine, theirs, where, at, size).start()

    def v_wait(turn):
        for mine, theirs, exists, where in sides:
            @pl.when(exists)
            def _():
                v_copy(turn, mine, theirs, where, 0, rows).wait_send()
                v_copy(turn, theirs, mine, where, 0, rows).wait_recv()

    def p_copy(mine, theirs, where, at, size):
        return pltpu.make_async_remote_copy(
            src_ref=p_t.at[pl.ds(at, size), pl.ds(0, rows)],
            dst_ref=p_t.at[pl.ds(at, size), pl.ds(theirs * slot, rows)],
            send_sem=p_send.at[mine], recv_sem=p_recv.at[theirs],
            device_id=where, device_id_type=MESH)

    def p_start(at, size):
        for mine, theirs, exists, where in sides:
            @pl.when(exists)
            def _():
                p_copy(mine, theirs, where, at, size).start()

    def p_wait():
        for mine, theirs, exists, where in sides:
            @pl.when(exists)
            def _():
                p_copy(mine, theirs, where, 0, ns).wait_send()
                p_copy(theirs, mine, where, 0, ns).wait_recv()

    def spread(own, table, send_sem, recv_sem):
        for where in others:
            pltpu.make_async_remote_copy(
                src_ref=own, dst_ref=table.at[me], send_sem=send_sem, recv_sem=recv_sem,
                device_id=where, device_id_type=MESH).start()

    def spread_wait(table, send_sem, recv_sem):
        part = table.at[pl.ds(0, n - 1)]
        pltpu.make_async_copy(part, part, send_sem).wait()
        pltpu.make_async_copy(part, part, recv_sem).wait()

    v_start(0, 0, rows)
    p0_copy.wait()
    first, second = ns // 3, 2 * ns // 3
    v_wait(0)
    p_start(0, first)

    lanes = lax.broadcasted_iota(jnp.int32, (width, width), 1)
    late = hold.shape[0]

    def lane_sum(total):
        return jnp.sum(total, axis=1, keepdims=True)

    def mix(turn, b):
        src = tables[1 - turn]
        total = a_v[b, 0] * src[b]
        for k in range(1, blocks):
            total = total + a_v[b, k] * src[cols_s[k, b]]
        return total

    def pair(turn, g, p):
        src = tables[1 - turn]
        b = g * group + vpu + 2 * p
        x = jnp.concatenate(
            [jnp.concatenate([src[b + i] if k == 0 else src[cols_s[k, b + i]]
                              for k in range(blocks)], axis=1) for i in range(2)], axis=0)
        hi = x.astype(jnp.bfloat16).astype(f32)
        left = jnp.concatenate([hi, x - hi, jnp.zeros((4, x.shape[1]), f32)], axis=0).astype(jnp.bfloat16)
        left = jnp.concatenate([left, left], axis=1)
        out = jnp.dot(left, w_t[g * pairs + p], preferred_element_type=f32)
        out = out[0:2] + out[2:4]
        for i in range(2):
            r = vpu + 2 * p + i
            tables[turn][b + i] = out[i:i + 1, i * width:(i + 1) * width] / diag[b + i]

    def mix_block(turn, g, size, count, first):
        if not first:
            for p in range(pairs):
                pair(turn, g, p)
        packed = jnp.zeros((width, width), f32)
        for r in range(count):
            b = g * size + r
            total = mix(turn, b)
            if r < count - late:
                packed = jnp.where(lanes == r, lane_sum(total), packed)
            else:
                hold[r - (count - late)] = total
            if first:
                eye = lanes == lax.broadcasted_iota(jnp.int32, (width, width), 0)
                diag[b] = jnp.sum(jnp.where(eye, a_v[b, 0], 0.0), axis=0, keepdims=True)
        s_v[...] = packed

    def finish_block(turn, g, size, count):
        packed = s_v[...]
        for i in range(late):
            packed = jnp.where(lanes == count - late + i, lane_sum(hold[i]), packed)
        out = packed.T
        for r in range(count):
            b = g * size + r
            tables[turn][b] = out[r:r + 1] / diag[b]

    def operate(turn, first, send):
        size, count = (load, load) if first else (group, vpu)
        if first:
            a_copy(0).wait()
        mix_block(turn, 0, size, count, first)

        def body(g, c):
            if first:
                a_copy(g).wait()
            finish_block(turn, g - 1, size, count)
            mix_block(turn, g, size, count, first)
            if send:
                v_start(turn, (g - 1) * size, size)
            return c

        lax.fori_loop(1, rows // size, body, 0)
        finish_block(turn, rows // size - 1, size, count)
        if send:
            v_start(turn, rows - size, size)

    def turn_over(i, c):
        b = i // pairs * group + vpu + 2 * lax.rem(i, pairs)
        for k in range(blocks):
            x = jnp.concatenate([a_v[b, k].T, a_v[b + 1, k].T], axis=1)
            hi = x.astype(jnp.bfloat16)
            lo = (x - hi.astype(f32)).astype(jnp.bfloat16)
            w_t[i, k * width:(k + 1) * width] = hi
            w_t[i, (blocks + k) * width:(blocks + k + 1) * width] = lo
        return c

    each = 2 - rows % 2

    def product(i, c):
        for b, k in [(i * each + r, k) for r in range(each) for k in range(blocks)]:
            at = b
            if k:
                col = cols_s[k, b]
                at = col + (slot - rows) * (col // rows)
            p = p_t[:, at, :]
            p = jnp.concatenate([p, jnp.zeros((8 - ns % 8, width), f32)], axis=0)
            hi = p.astype(jnp.bfloat16).astype(f32)
            left = jnp.concatenate([hi, p - hi], axis=0).astype(jnp.bfloat16)
            left = jnp.concatenate([left, left], axis=1)
            out = lax.dot_general(left, split_bf16(a_v[b, k]), NT, preferred_element_type=f32)
            half = out.shape[0] // 2
            q_v[k, :, b, :] = (out[:half] + out[half:])[:ns]
        return c

    def columns():
        counts = meta[...][:, :, width - 1:]
        owner = lax.broadcasted_iota(jnp.int32, counts.shape, 0)
        slots = [(jnp.bool_(True), me)]
        for (name, count, at, stride) in zip(AXES, sizes, (ix, iy, iz), (ny * nz, nz, 1)):
            slots.append((at > 0, me - stride))
            slots.append((at < count - 1, me + stride))
        entries = []
        for exists, d in slots:
            d = jnp.where(exists, d, me)
            offset = jnp.sum(jnp.where(owner < d, counts, 0).astype(f32), axis=0)
            entries.append(meta[d].astype(f32) + offset)
        entries.append(jnp.zeros((1, width), f32))
        table = jnp.concatenate(entries, axis=0).T
        row = lax.broadcasted_iota(jnp.int32, (rows, rows), 0)
        for k in range(blocks):
            cols = cols_v[k:k + 1]
            found = jnp.zeros((rows, rows), f32)
            for s in range(len(slots)):
                found = found + jnp.where(cols - s * rows == row, table[:rows, s:s + 1], 0.0)
            pcols_v[k:k + 1] = (jnp.sum(found, axis=0, keepdims=True) * ns).astype(jnp.int32)

    def squares(turn):
        own = tables[turn][0:rows]
        return jnp.sum(jnp.sum(own * own, axis=0), axis=1, keepdims=True)

    operate(1, True, True)
    lax.fori_loop(0, w_t.shape[0], turn_over, 0)
    p_start(first, second - first)
    v_wait(1)

    def step(t, turn):
        operate(turn, False, True)

        @pl.when(t == 3)
        def _():
            p_wait()
            own_v[...] = p_t[:, 0:rows]

        @pl.when(t >= 3)
        def _():
            lax.fori_loop(rows // each * (t - 3) // (ITERS - 3), rows // each * (t - 2) // (ITERS - 3), product, 0)

        @pl.when(t == ITERS - 1)
        def _():
            spread_wait(meta, m_send, m_recv)
            columns()

        v_wait(turn)

        @pl.when(t == 2)
        def _():
            p_start(second, ns - second)

        @pl.when(t == SPREAD)
        def _():
            spread(meta_own, meta, m_send, m_recv)

    def steps(i, c):
        for turn in range(2):
            step(2 * i + turn, turn)
        return c

    lax.fori_loop(1, ITERS // 2, steps, 0)
    before = squares((ITERS - 1) % 2)
    operate(ITERS % 2, False, False)

    lane = lax.broadcasted_iota(jnp.int32, (1, width), 1)
    sums_own[...] = jnp.where(lane == 0, before, jnp.where(lane == 1, squares(ITERS % 2), 0.0))
    sums[pl.ds(me, 1)] = sums_own[...][None]
    spread(sums_own, sums, s_send, s_recv)
    spread_wait(sums, s_send, s_recv)
    totals = jnp.sum(sums[...], axis=0)
    total_before = jnp.sum(jnp.where(lane == 0, totals, 0.0), axis=1, keepdims=True)
    total_last = jnp.sum(jnp.where(lane == 1, totals, 0.0), axis=1, keepdims=True)
    last_norm = jnp.sqrt(total_last)
    spectral = last_norm / jnp.sqrt(total_before)
    damping = 4.0 / (3.0 * spectral)
    factor = jnp.sqrt(jnp.full((1, 1), n * rows * width, f32)) / last_norm
    for r in range(rows):
        power_v[r:r + 1] = tables[ITERS % 2][r] * factor

    by_v[...] = -(damping / jnp.concatenate([diag[r] for r in range(rows)], axis=0))


def scale_kernel(q, p0, by, cols, power, p_hbm, cols_hbm, power_hbm, p_v, p_sem, sem):
    small = [pltpu.make_async_copy(a, b, sem.at[i]) for i, (a, b) in enumerate(((cols, cols_hbm), (power, power_hbm)))]
    for copy in small:
        copy.start()
    factor = by[...]
    copies = [pltpu.make_async_copy(p_v.at[k], p_hbm.at[k], p_sem.at[k]) for k in range(q.shape[0])]
    for k, copy in enumerate(copies):
        for c in range(q.shape[1]):
            scaled = factor * q[k, c]
            p_v[k, c] = scaled + p0[c] if k == 0 else scaled
        copy.start()
    for copy in small + copies:
        copy.wait()


def solution(mesh):
    sizes = tuple(mesh.shape[a] for a in AXES)
    n = sizes[0] * sizes[1] * sizes[2]

    def local(a_blocks, block_cols, agg_ids, agg_counts, p0_blocks, start_vec):
        rows, blocks, width, _ = a_blocks.shape
        ns = p0_blocks.shape[1]
        load = next(g for g in (13, 4, 2, 1) if rows % g == 0)
        group = 2 * load if rows % (2 * load) == 0 else load
        vpu = group - group * 4 // 13 // 2 * 2
        late = min(3, load, vpu)
        vmem = pl.BlockSpec(memory_space=pltpu.VMEM)
        dma = pltpu.SemaphoreType.DMA
        f32 = jnp.float32
        assert rows < width
        p0_planes = p0_blocks.transpose(1, 0, 2)
        hbm = pl.BlockSpec(memory_space=pl.ANY)
        product, own, cols, power, by = pl.pallas_call(
            functools.partial(kernel, sizes, (load, group, vpu)),
            out_shape=(
                pltpu.VMEM((blocks, ns, rows, width), f32),
                pltpu.VMEM((ns, rows, width), f32),
                pltpu.VMEM((blocks, rows), jnp.int32),
                pltpu.VMEM((rows, width), f32),
                pltpu.VMEM((rows, width), f32),
            ),
            in_specs=[pl.BlockSpec(memory_space=pltpu.HBM)] * 6,
            out_specs=(vmem,) * 5,
            scratch_shapes=[
                pltpu.SMEM((blocks, rows), jnp.int32),
                pltpu.VMEM((blocks, rows), jnp.int32),
                pltpu.VMEM((1, rows), jnp.int32),
                pltpu.SMEM((1,), jnp.int32),
                pltpu.VMEM((rows, width), f32),
                pltpu.VMEM((rows, blocks, width, width), f32),
                pltpu.VMEM((7 * rows, 1, width), f32),
                pltpu.VMEM((7 * rows, 1, width), f32),
                pltpu.VMEM((ns, 7 * (-(-rows // 8) * 8), width), f32),
                pltpu.VMEM((rows, 1, width), f32),
                pltpu.VMEM((rows // group * ((group - vpu) // 2), 2 * blocks * width, 2 * width), jnp.bfloat16),
                pltpu.VMEM((width, width), f32),
                pltpu.VMEM((late, width, width), f32),
                pltpu.VMEM((n, 1, width), jnp.int32),
                pltpu.VMEM((n, 1, width), f32),
                pltpu.VMEM((1, width), jnp.int32),
                pltpu.VMEM((1, width), f32),
                dma((rows // load,)), dma, dma((5,)),
                dma((2, 7)), dma((2, 7)), dma((7,)), dma((7,)),
                dma, dma, dma, dma,
            ],
            compiler_params=pltpu.CompilerParams(
                collective_id=0, has_side_effects=True, vmem_limit_bytes=(67043328 - 1470 * 1024)),
        )(a_blocks, block_cols.T, agg_ids[None], agg_counts, p0_planes, start_vec)
        product, cols, power = pl.pallas_call(
            scale_kernel,
            out_shape=(
                jax.ShapeDtypeStruct(product.shape, f32),
                jax.ShapeDtypeStruct(cols.shape, jnp.int32),
                jax.ShapeDtypeStruct(power.shape, f32),
            ),
            in_specs=[vmem] * 5,
            out_specs=(hbm,) * 3,
            scratch_shapes=[pltpu.VMEM(product.shape, f32), dma((blocks,)), dma((2,))],
            compiler_params=pltpu.CompilerParams(vmem_limit_bytes=8 * 1024 * 1024),
        )(product, own, by, cols, power)
        return product.transpose(2, 0, 1, 3), cols.T, power

    part = P(AXES)
    return jax.shard_map(
        local, mesh=mesh, in_specs=(part,) * 6, out_specs=(part,) * 3, check_vma=False)
```

```python
import functools

import jax
import jax.numpy as jnp
from jax import lax
from jax.experimental import pallas as pl
from jax.experimental.pallas import tpu as pltpu
from jax.sharding import PartitionSpec as P

ITERS = 8
SPREAD = ITERS - 3
AXES = ("gx", "gy", "gz")
MESH = pl.DeviceIdType.MESH
NT = (((1,), (1,)), ((), ()))


def split_bf16(x):
    hi = x.astype(jnp.bfloat16)
    lo = (x - hi.astype(jnp.float32)).astype(jnp.bfloat16)
    return jnp.concatenate([hi, lo], axis=1)


def kernel(sizes, plan, a_hbm, cols_hbm, ids_hbm, count_hbm, p0_hbm, start_hbm,
           q_v, own_v, pcols_v, power_v, by_v,
           cols_s, cols_v, ids_v, count_s, start_v, a_v, va, vb, p_t, diag, w_t, s_v, hold, meta, sums, meta_own, sums_own,
           a_sem, p0_sem, in_sem, v_send, v_recv, p_send, p_recv, m_send, m_recv, s_send, s_recv):
    nx, ny, nz = sizes
    n = nx * ny * nz
    rows, blocks, width, _ = a_v.shape
    ns = p0_hbm.shape[0]
    slot = p_t.shape[1] // 7
    ix, iy, iz = (lax.axis_index(a) for a in AXES)
    me = (ix * ny + iy) * nz + iz
    load, group, vpu = plan
    pairs = (group - vpu) // 2
    f32 = jnp.float32

    def a_copy(g):
        return pltpu.make_async_copy(
            a_hbm.at[pl.ds(g * load, load)], a_v.at[pl.ds(g * load, load)], a_sem.at[g])

    p0_copy = pltpu.make_async_copy(p0_hbm, p_t.at[:, pl.ds(0, rows)], p0_sem)
    inputs = [pltpu.make_async_copy(a, b, in_sem.at[i]) for i, (a, b) in enumerate((
        (start_hbm, start_v), (ids_hbm, ids_v), (count_hbm, count_s), (cols_hbm, cols_s), (cols_hbm, cols_v)))]
    for copy in inputs:
        copy.start()
    p0_copy.start()
    for g in range(rows // load):
        a_copy(g).start(priority=1)

    others = []
    for dx in range(nx):
        for dy in range(ny):
            for dz in range(nz):
                if dx or dy or dz:
                    others.append(((dx > 0) + (dy > 0), {
                        "gx": lax.rem(ix + dx, nx), "gy": lax.rem(iy + dy, ny), "gz": lax.rem(iz + dz, nz)}))
    others = [where for _, where in sorted(others, key=lambda o: -o[0])]

    sides = []
    for axis, (name, count, at) in enumerate(zip(AXES, sizes, (ix, iy, iz))):
        if count > 1:
            sides.append((2 * axis + 1, 2 * axis + 2, at > 0, {name: at - 1}))
            sides.append((2 * axis + 2, 2 * axis + 1, at < count - 1, {name: at + 1}))

    near = nx + ny + nz - 3 <= SPREAD + 2
    barrier = pltpu.get_barrier_semaphore()
    if near:
        for _, _, exists, where in sides:
            @pl.when(exists)
            def _():
                pl.semaphore_signal(barrier, inc=1, device_id=where, device_id_type=MESH)
    else:
        for where in others:
            pl.semaphore_signal(barrier, inc=1, device_id=where, device_id_type=MESH)

    for copy in inputs:
        copy.wait()
    for r in range(rows):
        va[r] = start_v[r:r + 1]
    meta_own[0:1] = jnp.full((1, width), count_s[0], jnp.int32)
    meta_own[0:1, 0:rows] = ids_v[...]
    meta[pl.ds(me, 1)] = meta_own[...][None]
    if near:
        pl.semaphore_wait(barrier, sum(exists.astype(jnp.int32) for _, _, exists, _ in sides))
    else:
        pl.semaphore_wait(barrier, n - 1)

    tables = (va, vb)

    def v_copy(turn, mine, theirs, where, at, size):
        table = tables[turn]
        return pltpu.make_async_remote_copy(
            src_ref=table.at[pl.ds(at, size)],
            dst_ref=table.at[pl.ds(theirs * rows + at, size)],
            send_sem=v_send.at[turn, mine], recv_sem=v_recv.at[turn, theirs],
            device_id=where, device_id_type=MESH)

    def v_start(turn, at, size):
        for mine, theirs, exists, where in sides:
            @pl.when(exists)
            def _():
                v_copy(turn, mine, theirs, where, at, size).start()

    def v_wait(turn):
        for mine, theirs, exists, where in sides:
            @pl.when(exists)
            def _():
                v_copy(turn, mine, theirs, where, 0, rows).wait_send()
                v_copy(turn, theirs, mine, where, 0, rows).wait_recv()

    def p_copy(mine, theirs, where, at, size):
        return pltpu.make_async_remote_copy(
            src_ref=p_t.at[pl.ds(at, size), pl.ds(0, rows)],
            dst_ref=p_t.at[pl.ds(at, size), pl.ds(theirs * slot, rows)],
            send_sem=p_send.at[mine], recv_sem=p_recv.at[theirs],
            device_id=where, device_id_type=MESH)

    def p_start(at, size):
        for mine, theirs, exists, where in sides:
            @pl.when(exists)
            def _():
                p_copy(mine, theirs, where, at, size).start()

    def p_wait():
        for mine, theirs, exists, where in sides:
            @pl.when(exists)
            def _():
                p_copy(mine, theirs, where, 0, ns).wait_send()
                p_copy(theirs, mine, where, 0, ns).wait_recv()

    def spread(own, table, send_sem, recv_sem):
        for where in others:
            pltpu.make_async_remote_copy(
                src_ref=own, dst_ref=table.at[me], send_sem=send_sem, recv_sem=recv_sem,
                device_id=where, device_id_type=MESH).start()

    def spread_wait(table, send_sem, recv_sem):
        part = table.at[pl.ds(0, n - 1)]
        pltpu.make_async_copy(part, part, send_sem).wait()
        pltpu.make_async_copy(part, part, recv_sem).wait()

    v_start(0, 0, rows)
    p0_copy.wait()
    first, second = ns // 3, 2 * ns // 3
    v_wait(0)
    p_start(0, first)

    lanes = lax.broadcasted_iota(jnp.int32, (width, width), 1)
    late = hold.shape[0]

    def lane_sum(total):
        return jnp.sum(total, axis=1, keepdims=True)

    def mix(turn, b):
        src = tables[1 - turn]
        total = a_v[b, 0] * src[b]
        for k in range(1, blocks):
            total = total + a_v[b, k] * src[cols_s[k, b]]
        return total

    def pair(turn, g, p):
        src = tables[1 - turn]
        b = g * group + vpu + 2 * p
        x = jnp.concatenate(
            [jnp.concatenate([src[b + i] if k == 0 else src[cols_s[k, b + i]]
                              for k in range(blocks)], axis=1) for i in range(2)], axis=0)
        hi = x.astype(jnp.bfloat16).astype(f32)
        left = jnp.concatenate([hi, x - hi, jnp.zeros((4, x.shape[1]), f32)], axis=0).astype(jnp.bfloat16)
        left = jnp.concatenate([left, left], axis=1)
        out = jnp.dot(left, w_t[g * pairs + p], preferred_element_type=f32)
        out = out[0:2] + out[2:4]
        for i in range(2):
            r = vpu + 2 * p + i
            tables[turn][b + i] = out[i:i + 1, i * width:(i + 1) * width] / diag[b + i]

    def mix_block(turn, g, size, count, first):
        if not first:
            for p in range(pairs):
                pair(turn, g, p)
        packed = jnp.zeros((width, width), f32)
        for r in range(count):
            b = g * size + r
            total = mix(turn, b)
            if r < count - late:
                packed = jnp.where(lanes == r, lane_sum(total), packed)
            else:
                hold[r - (count - late)] = total
            if first:
                eye = lanes == lax.broadcasted_iota(jnp.int32, (width, width), 0)
                diag[b] = jnp.sum(jnp.where(eye, a_v[b, 0], 0.0), axis=0, keepdims=True)
        s_v[...] = packed

    def finish_block(turn, g, size, count):
        packed = s_v[...]
        for i in range(late):
            packed = jnp.where(lanes == count - late + i, lane_sum(hold[i]), packed)
        out = packed.T
        for r in range(count):
            b = g * size + r
            tables[turn][b] = out[r:r + 1] / diag[b]

    def operate(turn, first, send):
        size, count = (load, load) if first else (group, vpu)
        if first:
            a_copy(0).wait()
        mix_block(turn, 0, size, count, first)

        def body(g, c):
            if first:
                a_copy(g).wait()
            finish_block(turn, g - 1, size, count)
            mix_block(turn, g, size, count, first)
            if first:
                v_start(turn, (g - 1) * size, size)
            return c

        lax.fori_loop(1, rows // size, body, 0)
        finish_block(turn, rows // size - 1, size, count)
        if first:
            v_start(turn, rows - size, size)
        else:
            if send is not True:
                pl.when(send)(lambda: v_start(turn, 0, rows))
            else:
                v_start(turn, 0, rows)

    def turn_over(i, c):
        b = i // pairs * group + vpu + 2 * lax.rem(i, pairs)
        for k in range(blocks):
            x = jnp.concatenate([a_v[b, k].T, a_v[b + 1, k].T], axis=1)
            hi = x.astype(jnp.bfloat16)
            lo = (x - hi.astype(f32)).astype(jnp.bfloat16)
            w_t[i, k * width:(k + 1) * width] = hi
            w_t[i, (blocks + k) * width:(blocks + k + 1) * width] = lo
        return c

    each = 2 - rows % 2

    def product(i, c):
        for b, k in [(i * each + r, k) for r in range(each) for k in range(blocks)]:
            at = b
            if k:
                col = cols_s[k, b]
                at = col + (slot - rows) * (col // rows)
            p = p_t[:, at, :]
            p = jnp.concatenate([p, jnp.zeros((8 - ns % 8, width), f32)], axis=0)
            hi = p.astype(jnp.bfloat16).astype(f32)
            left = jnp.concatenate([hi, p - hi], axis=0).astype(jnp.bfloat16)
            left = jnp.concatenate([left, left], axis=1)
            out = lax.dot_general(left, split_bf16(a_v[b, k]), NT, preferred_element_type=f32)
            half = out.shape[0] // 2
            q_v[k, :, b, :] = (out[:half] + out[half:])[:ns]
        return c

    def columns():
        counts = meta[...][:, :, width - 1:]
        owner = lax.broadcasted_iota(jnp.int32, counts.shape, 0)
        slots = [(jnp.bool_(True), me)]
        for (name, count, at, stride) in zip(AXES, sizes, (ix, iy, iz), (ny * nz, nz, 1)):
            slots.append((at > 0, me - stride))
            slots.append((at < count - 1, me + stride))
        entries = []
        for exists, d in slots:
            d = jnp.where(exists, d, me)
            offset = jnp.sum(jnp.where(owner < d, counts, 0).astype(f32), axis=0)
            entries.append(meta[d].astype(f32) + offset)
        entries.append(jnp.zeros((1, width), f32))
        table = jnp.concatenate(entries, axis=0).T
        row = lax.broadcasted_iota(jnp.int32, (rows, rows), 0)
        for k in range(blocks):
            cols = cols_v[k:k + 1]
            found = jnp.zeros((rows, rows), f32)
            for s in range(len(slots)):
                found = found + jnp.where(cols - s * rows == row, table[:rows, s:s + 1], 0.0)
            pcols_v[k:k + 1] = (jnp.sum(found, axis=0, keepdims=True) * ns).astype(jnp.int32)

    def squares(turn):
        own = tables[turn][0:rows]
        return jnp.sum(jnp.sum(own * own, axis=0), axis=1, keepdims=True)

    operate(1, True, True)
    lax.fori_loop(0, w_t.shape[0], turn_over, 0)
    p_start(first, second - first)
    v_wait(1)

    def between(t, turn):
        @pl.when(t == 3)
        def _():
            p_wait()
            own_v[...] = p_t[:, 0:rows]

        @pl.when(t >= 3)
        def _():
            lax.fori_loop(rows // each * (t - 3) // (ITERS - 3), rows // each * (t - 2) // (ITERS - 3), product, 0)

        @pl.when(t == ITERS - 1)
        def _():
            spread_wait(meta, m_send, m_recv)
            columns()

        v_wait(turn)

        @pl.when(t == 2)
        def _():
            p_start(second, ns - second)

        @pl.when(t == SPREAD)
        def _():
            spread(meta_own, meta, m_send, m_recv)

    def steps(i, c):
        operate(0, False, i < ITERS // 2)

        @pl.when(i < ITERS // 2)
        def _():
            between(2 * i, 0)
            operate(1, False, True)
            between(2 * i + 1, 1)

        return c

    lax.fori_loop(1, ITERS // 2 + 1, steps, 0)
    before = squares((ITERS - 1) % 2)
    lane = lax.broadcasted_iota(jnp.int32, (1, width), 1)
    sums_own[...] = jnp.where(lane == 0, before, jnp.where(lane == 1, squares(ITERS % 2), 0.0))
    sums[pl.ds(me, 1)] = sums_own[...][None]
    spread(sums_own, sums, s_send, s_recv)
    spread_wait(sums, s_send, s_recv)
    totals = jnp.sum(sums[...], axis=0)
    total_before = jnp.sum(jnp.where(lane == 0, totals, 0.0), axis=1, keepdims=True)
    total_last = jnp.sum(jnp.where(lane == 1, totals, 0.0), axis=1, keepdims=True)
    last_norm = jnp.sqrt(total_last)
    spectral = last_norm / jnp.sqrt(total_before)
    damping = 4.0 / (3.0 * spectral)
    factor = jnp.sqrt(jnp.full((1, 1), n * rows * width, f32)) / last_norm
    for r in range(rows):
        power_v[r:r + 1] = tables[ITERS % 2][r] * factor

    by_v[...] = -(damping / jnp.concatenate([diag[r] for r in range(rows)], axis=0))


def scale_kernel(q, p0, by, cols, power, p_hbm, cols_hbm, power_hbm, p_v, p_sem, sem):
    small = [pltpu.make_async_copy(a, b, sem.at[i]) for i, (a, b) in enumerate(((cols, cols_hbm), (power, power_hbm)))]
    for copy in small:
        copy.start()
    factor = by[...]
    copies = [pltpu.make_async_copy(p_v.at[k], p_hbm.at[k], p_sem.at[k]) for k in range(q.shape[0])]
    for k, copy in enumerate(copies):
        for c in range(q.shape[1]):
            scaled = factor * q[k, c]
            p_v[k, c] = scaled + p0[c] if k == 0 else scaled
        copy.start()
    for copy in small + copies:
        copy.wait()


def solution(mesh):
    sizes = tuple(mesh.shape[a] for a in AXES)
    n = sizes[0] * sizes[1] * sizes[2]

    def local(a_blocks, block_cols, agg_ids, agg_counts, p0_blocks, start_vec):
        rows, blocks, width, _ = a_blocks.shape
        ns = p0_blocks.shape[1]
        load = next(g for g in (26, 4, 2, 1) if rows % g == 0)
        group = next(g for g in (26, 13, 4, 2, 1) if rows % g == 0)
        vpu = group - group * 3 // 13 // 2 * 2
        late = min(3, load, vpu)
        vmem = pl.BlockSpec(memory_space=pltpu.VMEM)
        dma = pltpu.SemaphoreType.DMA
        f32 = jnp.float32
        assert rows < width
        p0_planes = p0_blocks.transpose(1, 0, 2)
        hbm = pl.BlockSpec(memory_space=pl.ANY)
        product, own, cols, power, by = pl.pallas_call(
            functools.partial(kernel, sizes, (load, group, vpu)),
            out_shape=(
                pltpu.VMEM((blocks, ns, rows, width), f32),
                pltpu.VMEM((ns, rows, width), f32),
                pltpu.VMEM((blocks, rows), jnp.int32),
                pltpu.VMEM((rows, width), f32),
                pltpu.VMEM((rows, width), f32),
            ),
            in_specs=[pl.BlockSpec(memory_space=pltpu.HBM)] * 6,
            out_specs=(vmem,) * 5,
            scratch_shapes=[
                pltpu.SMEM((blocks, rows), jnp.int32),
                pltpu.VMEM((blocks, rows), jnp.int32),
                pltpu.VMEM((1, rows), jnp.int32),
                pltpu.SMEM((1,), jnp.int32),
                pltpu.VMEM((rows, width), f32),
                pltpu.VMEM((rows, blocks, width, width), f32),
                pltpu.VMEM((7 * rows, 1, width), f32),
                pltpu.VMEM((7 * rows, 1, width), f32),
                pltpu.VMEM((ns, 7 * (-(-rows // 8) * 8), width), f32),
                pltpu.VMEM((rows, 1, width), f32),
                pltpu.VMEM((rows // group * ((group - vpu) // 2), 2 * blocks * width, 2 * width), jnp.bfloat16),
                pltpu.VMEM((width, width), f32),
                pltpu.VMEM((late, width, width), f32),
                pltpu.VMEM((n, 1, width), jnp.int32),
                pltpu.VMEM((n, 1, width), f32),
                pltpu.VMEM((1, width), jnp.int32),
                pltpu.VMEM((1, width), f32),
                dma((rows // load,)), dma, dma((5,)),
                dma((2, 7)), dma((2, 7)), dma((7,)), dma((7,)),
                dma, dma, dma, dma,
            ],
            compiler_params=pltpu.CompilerParams(
                collective_id=0, has_side_effects=True, vmem_limit_bytes=(67043328 - 1470 * 1024)),
        )(a_blocks, block_cols.T, agg_ids[None], agg_counts, p0_planes, start_vec)
        product, cols, power = pl.pallas_call(
            scale_kernel,
            out_shape=(
                jax.ShapeDtypeStruct(product.shape, f32),
                jax.ShapeDtypeStruct(cols.shape, jnp.int32),
                jax.ShapeDtypeStruct(power.shape, f32),
            ),
            in_specs=[vmem] * 5,
            out_specs=(hbm,) * 3,
            scratch_shapes=[pltpu.VMEM(product.shape, f32), dma((blocks,)), dma((2,))],
            compiler_params=pltpu.CompilerParams(vmem_limit_bytes=8 * 1024 * 1024),
        )(product, own, by, cols, power)
        return product.transpose(2, 0, 1, 3), cols.T, power

    part = P(AXES)
    return jax.shard_map(
        local, mesh=mesh, in_specs=(part,) * 6, out_specs=(part,) * 3, check_vma=False)
```
